32 devices in a mesh: row: 4 (over y, x), col: 8 (over z, core).
Axes of the slice: x: 2, y: 2, z: 4, core: 2. Of those that a mesh axis runs over, the one named last changes fastest.
Arguments:
- psi: bfloat16 [8192, 8192], P(('row', 'col')), may hold values from -0.125 to 0.125
- hpsi: bfloat16 [8192, 128], P(('row', 'col')), may hold values from -0.796875 to 0.796875
- slab_counts: int32 [32], P(('row', 'col')), may hold values from 1 to 256, 6144 in all
- matrix: float32 [4, 2048, 8, 1024], P('row', None, 'col'), as said below
Outputs:
- reduced: float32 [4, 2048, 8, 1024], P('row', None, 'col')
The draws below stay inside these ranges and needn't reach their ends.
Inputs may be any that keep to these rules, and one draw needn't show every extreme that they name: Slab k's live plane waves are its first slab_counts[k] slots; the rest are padding; the counts sum to 3 * 256 * 32 // 4. The stored matrix is symmetric.
All inputs are finite; a program needn't handle non-finite values.
Results may differ from the reference program's by a relative error of at most 0.0003.
Values sent between devices are 32-bit elements; how exact they have to be, the bound alone decides.
No kernel may reach another device: no remote copies, remote signals or barrier semaphores. Data moves between devices by JAX's collectives and lax.ppermute only.
A program may use at most 64 MiB of HBM per device.

```python
import math
import jax
import jax.numpy as jnp
import numpy as np
from jax import lax

NB = 8192
PANEL = 128
TILE = 16
G_DEV = 256
NG = 8192
N_ROW = 4
N_COL = 8
DEVICES = 32


def draw_matrix(key, part):
    first = jax.random.normal(jax.random.fold_in(key, 11), (NB, NB), jnp.float32)
    sym = (first + first.T) * 0.7071
    tiles_r = NB // (TILE * N_ROW)
    tiles_c = NB // (TILE * N_COL)
    grid = sym.reshape(tiles_r, N_ROW, TILE, tiles_c, N_COL, TILE)
    return grid.transpose(1, 0, 2, 4, 3, 5).reshape(N_ROW, NB // N_ROW, N_COL, NB // N_COL)


def raised(drawn, key, source, target, shards_of, factor):
    def block_of(axis_at):
        return (jnp.arange(drawn.shape[axis_at]) // (drawn.shape[axis_at] // shards_of)).reshape((-1,) + (1,) * (drawn.ndim - 1 - axis_at))

    near = jax.random.permutation(key, shards_of)[block_of(target)]
    second = (block_of(target) + shards_of // 2) % shards_of
    return jnp.where((block_of(source) == near) | (block_of(source) == second), factor * drawn, drawn)


def shard_levels(stream_key, shape, split, low, high):
    loudness = 1.0
    for position, parts in split:
        heights = jax.random.uniform(jax.random.fold_in(jax.random.fold_in(stream_key, 6), position), (parts,), jnp.float32, low / len(split), high / len(split))
        loudness = loudness * jnp.repeat(jnp.exp(heights), shape[position] // parts).reshape((-1,) + (1,) * (len(shape) - 1 - position))
    return loudness


def profile(amount, total, limit, slope):
    weights = [(1 << 20) // math.isqrt(grade ** slope) + 1 for grade in range(2, amount + 1)]
    surplus, given = total - limit - (amount - 1), [1] * (amount - 1)
    while surplus > 0:
        candidates = [i for i in range(amount - 1) if given[i] < limit]
        whole, left = sum([weights[i] for i in candidates]), surplus
        for i in candidates:
            more = min(limit - given[i], max(1, left * weights[i] // whole), surplus)
            given[i] = given[i] + more
            surplus = surplus - more
    return np.array([limit] + given)


def uneven_parts(own_key, number_of, total, limit, slope):
    if number_of == 2:
        one = jax.random.randint(own_key, (), max(1, total - limit), min(limit, total - 1) + 1)
        return jnp.stack([one, total - one])
    lengths = jnp.asarray(profile(number_of, total, limit, slope), jnp.int32)
    couples = (number_of - 1) // 2
    source_of, sink = lengths[1:1 + 2 * couples:2], lengths[2:2 + 2 * couples:2]
    margin = jnp.minimum(source_of - 1, limit - sink)
    passed = jax.random.randint(jax.random.fold_in(own_key, 1), (couples,), 0, 1 << 20) % (margin + 1)
    lengths = lengths.at[1:1 + 2 * couples:2].set(source_of - passed).at[2:2 + 2 * couples:2].set(sink + passed)
    return lengths[jax.random.permutation(jax.random.fold_in(own_key, 2), number_of)]


def normal_values(key, dims, scale, most, shards=(), kind=jnp.bfloat16):
    entries = jax.random.normal(key, dims, jnp.float32) * scale
    if len(shards) > 0:
        entries = shard_levels(key, dims, shards, -0.22, 0.18) * entries
    return jnp.clip(entries, min=-most, max=most).astype(kind)


def heavy_noise(key, shape, spread, reach, cuts, heavy, kind=jnp.bfloat16):
    result = spread * jax.random.normal(key, shape, jnp.float32)
    if cuts:
        result = result * shard_levels(key, shape, cuts, -0.22, 0.18)
    return jnp.clip(raised(result, jax.random.fold_in(key, 3), *heavy), -reach, reach).astype(kind)


def setup_inputs(seed: int = 0) -> dict:
    keys = jax.random.split(jax.random.key(seed), 5)
    return {
        "psi": heavy_noise(keys[0], (NG, NB), NG ** -0.5, 0.125, ((0, 32),), (0, 1, 32, 2.75)),
        "hpsi": normal_values(keys[1], (NG, PANEL), 0.1, 0.796875, ((0, 32),)),
        "slab_counts": uneven_parts(keys[2], DEVICES, 3 * G_DEV * DEVICES // 4, G_DEV, 1).astype(jnp.int32),
        "matrix": draw_matrix(jax.random.fold_in(keys[4], 71), 0),
    }


HIGH = lax.Precision.HIGHEST

def to_full(stored):
    tiles_r = NB // (TILE * N_ROW)
    tiles_c = NB // (TILE * N_COL)
    grid = stored.reshape(N_ROW, tiles_r, TILE, N_COL, tiles_c, TILE)
    return grid.transpose(1, 0, 2, 4, 3, 5).reshape(NB, NB)

def to_stored(full):
    tiles_r = NB // (TILE * N_ROW)
    tiles_c = NB // (TILE * N_COL)
    grid = full.reshape(tiles_r, N_ROW, TILE, tiles_c, N_COL, TILE)
    return grid.transpose(1, 0, 2, 4, 3, 5).reshape(N_ROW, NB // N_ROW, N_COL, NB // N_COL)

def lower_solve(factor, rhs):
    return lax.linalg.triangular_solve(factor, rhs, left_side=True, lower=True)

def invert_shifted(shifted):
    normal = jnp.dot(shifted.T, shifted, precision=HIGH)
    factor = jnp.linalg.cholesky(normal)
    first = lower_solve(factor, shifted.T)
    return lax.linalg.triangular_solve(factor, first, left_side=True, lower=True, transpose_a=True)

def reference(psi, hpsi, slab_counts, matrix):
    valid = (jnp.arange(G_DEV, dtype=jnp.int32)[None, :] < slab_counts[:, None]).reshape(-1)
    hcols = jnp.where(valid[:, None], hpsi, jnp.zeros_like(hpsi))
    columns = lax.dot_general(psi.astype(jnp.float32), hcols.astype(jnp.float32), (((0,), (0,)), ((), ())), preferred_element_type=jnp.float32)
    full = to_full(matrix)
    corner = columns[:PANEL]
    refreshed = full.at[:, :PANEL].set(columns).at[:PANEL, :].set(columns.T)
    refreshed = refreshed.at[:PANEL, :PANEL].set(0.5 * (corner + corner.T))
    index = jnp.arange(NB, dtype=jnp.int32)
    lower = jnp.where((index >= PANEL)[:, None], columns, jnp.zeros_like(columns))
    gram = jnp.dot(lower.T, lower, precision=HIGH)
    factor = jnp.linalg.cholesky(gram)
    basis = lower_solve(factor, lower.T).T
    top = basis[PANEL:2 * PANEL]
    inverse = invert_shifted(jnp.eye(PANEL, dtype=jnp.float32) - top)
    embed = (index[:, None] == PANEL + jnp.arange(PANEL, dtype=jnp.int32)[None, :]).astype(jnp.float32)
    reflect = basis - embed
    zrows = jnp.dot(refreshed, reflect, precision=HIGH)
    ucols = jnp.dot(refreshed.T, reflect, precision=HIGH)
    wmat = jnp.dot(reflect.T, zrows, precision=HIGH)
    core = jnp.dot(jnp.dot(inverse, wmat, precision=HIGH), inverse.T, precision=HIGH)
    first = jnp.dot(reflect, jnp.dot(inverse, ucols.T, precision=HIGH), precision=HIGH)
    second = jnp.dot(jnp.dot(zrows, inverse.T, precision=HIGH) - jnp.dot(reflect, core, precision=HIGH), reflect.T, precision=HIGH)
    return to_stored(refreshed - first - second)
```

```python
import math

import jax
import jax.numpy as jnp
from jax import lax
from jax.experimental import pallas as pl
from jax.experimental.pallas import tpu as pltpu
from jax.sharding import PartitionSpec as P

TILE = 16
HIGH = lax.Precision.HIGH
HIGHEST = lax.Precision.HIGHEST
BOTH = ("row", "col")


def mm(a, b, precision=HIGHEST):
    return jnp.dot(a, b, precision=precision, preferred_element_type=jnp.float32)


def mm_t(a, b, precision=HIGHEST):
    return lax.dot_general(
        a, b, (((0,), (0,)), ((), ())), precision=precision, preferred_element_type=jnp.float32
    )


def mm_nt(a, b, precision=HIGHEST):
    return lax.dot_general(
        a, b, (((1,), (1,)), ((), ())), precision=precision, preferred_element_type=jnp.float32
    )


def swap(x, axis, mask):
    size = lax.axis_size(axis)
    return lax.ppermute(x, axis, [(i, i ^ mask) for i in range(size)])


def halve(x, dim, bit, axis, mask):
    send = lax.dynamic_index_in_dim(x, 1 - bit, dim, keepdims=False)
    keep = lax.dynamic_index_in_dim(x, bit, dim, keepdims=False)
    return keep + swap(send, axis, mask)


def join(own, other, bit, dim):
    first = jnp.where(bit == 0, own, other)
    second = jnp.where(bit == 0, other, own)
    return jnp.stack([first, second], axis=dim)


def double(x, dim, bit, axis, mask):
    return join(x, swap(x, axis, mask), bit, dim)


def sum_over(x, axis, streams=1):
    bits = int(math.log2(lax.axis_size(axis)))
    parts = jnp.split(x, streams, axis=0) if streams > 1 else [x]
    for step in range(bits):
        parts = [
            part + swap(part, axis, 1 << ((step + s) % bits)) for s, part in enumerate(parts)
        ]
    return jnp.concatenate(parts, axis=0) if streams > 1 else parts[0]


def lower_solve(factor, rhs):
    return lax.linalg.triangular_solve(factor, rhs, left_side=True, lower=True)


def invert_shifted(shifted):
    normal = mm_t(shifted, shifted)
    factor = jnp.linalg.cholesky(normal)
    first = lower_solve(factor, shifted.T)
    return lax.linalg.triangular_solve(factor, first, left_side=True, lower=True, transpose_a=True)


def split(x):
    high = x.astype(jnp.bfloat16)
    return high, (x - high.astype(jnp.float32)).astype(jnp.bfloat16)


def nt(a, b):
    return lax.dot_general(a, b, (((1,), (1,)), ((), ())), preferred_element_type=jnp.float32)


def update_kernel(blocks, m_ref, left_ref, right_ref, edge_rows_ref, edge_cols_ref, o_ref, buf, in_sem, out_sem):
    rows = buf.shape[0] // blocks
    edge_r = edge_rows_ref.shape[0]
    edge_c = edge_cols_ref.shape[1]

    def load(i):
        at = pl.ds(i * rows, rows)
        return pltpu.make_async_copy(m_ref.at[0, at, 0, :], buf.at[at, :], in_sem.at[i])

    def store(i):
        at = pl.ds(i * rows, rows)
        return pltpu.make_async_copy(buf.at[at, :], o_ref.at[0, at, 0, :], out_sem.at[i])

    for i in range(blocks):
        load(i).start()
    right_high, right_low = split(right_ref[...])
    for i in range(blocks):
        at = pl.ds(i * rows, rows)
        left_high, left_low = split(left_ref[at, :])
        term = nt(left_high, right_high) + (nt(left_high, right_low) + nt(left_low, right_high))
        load(i).wait()
        buf[at, :edge_c] = edge_cols_ref[at, :]
        if i == 0:
            buf[:edge_r, :] = edge_rows_ref[...]
        buf[at, :] = buf[at, :] - term
        store(i).start()
    for i in range(blocks):
        store(i).wait()


def update(matrix, left, right, edge_rows, edge_cols):
    rows, cols = matrix.shape[1], matrix.shape[3]
    blocks = max(1, rows // 256)
    vmem = pl.BlockSpec(memory_space=pltpu.VMEM)
    anywhere = pl.BlockSpec(memory_space=pl.ANY)
    import functools

    return pl.pallas_call(
        functools.partial(update_kernel, blocks),
        out_shape=jax.ShapeDtypeStruct(matrix.shape, jnp.float32),
        in_specs=[anywhere, vmem, vmem, vmem, vmem],
        out_specs=anywhere,
        scratch_shapes=[
            pltpu.VMEM((rows, cols), jnp.float32),
            pltpu.SemaphoreType.DMA((blocks,)),
            pltpu.SemaphoreType.DMA((blocks,)),
        ],
        compiler_params=pltpu.CompilerParams(vmem_limit_bytes=40 << 20),
        cost_estimate=pl.CostEstimate(
            flops=6 * rows * cols * left.shape[1], bytes_accessed=8 * rows * cols, transcendentals=0
        ),
    )(matrix, left, right, edge_rows, edge_cols)


def per_device(psi, hpsi, slab_counts, matrix):
    p = lax.axis_index("row")
    q = lax.axis_index("col")
    n_row = lax.axis_size("row")
    n_col = lax.axis_size("col")
    fold = n_col // n_row
    if n_col % n_row or fold != 2 or n_row & (n_row - 1) or n_row < 2:
        raise ValueError("mesh shape")
    low, high = q % n_row, q // n_row
    slots, bands = psi.shape
    panel = hpsi.shape[1]
    local_rows, local_cols = matrix.shape[1], matrix.shape[3]
    tiles_r, tiles_c = local_rows // TILE, local_cols // TILE
    row_bits = int(math.log2(n_row))
    panel_tiles = panel // TILE

    local_r = jnp.arange(local_rows, dtype=jnp.int32)
    local_c = jnp.arange(local_cols, dtype=jnp.int32)
    row_global = (local_r // TILE * n_row + p) * TILE + local_r % TILE
    col_global = (local_c // TILE * n_col + q) * TILE + local_c % TILE
    span = jnp.arange(panel, dtype=jnp.int32)

    valid = jnp.arange(slots, dtype=jnp.int32) < slab_counts[0]
    hcols = jnp.where(valid[:, None], hpsi, jnp.zeros_like(hpsi))
    term = lax.dot_general(
        psi, hcols, (((0,), (0,)), ((), ())), preferred_element_type=jnp.float32
    )
    rest = tiles_c // n_row
    block = TILE * panel
    low_bit = [(low >> i) & 1 for i in range(row_bits)]
    row_bit = [(p >> i) & 1 for i in range(row_bits)]
    s = term.reshape((2,) * row_bits + (rest, fold) + (2,) * row_bits + (TILE, panel))
    s = halve(s, row_bits - 1, low_bit[0], "col", 1)
    lead = row_bits - 1
    streams = 2 if rest % 2 == 0 else 1
    parts = jnp.split(s, streams, axis=lead)
    done = []
    orders = [[(i + k) % row_bits for i in range(row_bits)] for k in range(streams)]
    left_dims = [list(range(row_bits - 1, -1, -1)) for _ in range(streams)]
    for step in range(row_bits):
        for k in range(streams):
            b = orders[k][step]
            dim = lead + 2 + left_dims[k].index(b)
            left_dims[k].remove(b)
            parts[k] = halve(parts[k], dim, row_bit[b], "row", 1 << b)
    s = jnp.concatenate(parts, axis=lead)
    for b in range(1, row_bits):
        s = halve(s, row_bits - 1 - b, low_bit[b], "col", 1 << b)
    s = halve(s, 1, high, "col", n_row)
    for b in range(row_bits - 1, 0, -1):
        s = double(s, 0 if b == row_bits - 1 else row_bits - 1 - b, low_bit[b], "col", 1 << b)
    s = double(s, row_bits - 1, low_bit[0], "col", 1)
    own_cols = s.reshape(tiles_c, TILE, panel)
    s_r = double(own_cols, 1, high, "col", n_row).reshape(local_rows, panel)

    def across(x):
        halves = list(jnp.split(x, 2, axis=0))
        for k in range(2):
            held = [0]
            for step in range(row_bits):
                mask = 1 << ((step + k) % row_bits)
                pairs = [
                    ((c % n_row ^ d) * n_col + c, (c % n_row ^ d ^ mask) * n_col + c)
                    for c in range(n_col)
                    for d in held
                ]
                other = lax.ppermute(halves[k], BOTH, pairs)
                halves[k] = jnp.where(((p ^ low) & mask) != 0, other, halves[k])
                held = held + [d ^ mask for d in held]
        return jnp.concatenate(halves, axis=0)

    s_c = across(own_cols).reshape(local_cols, panel)

    def along(x):
        pairs = [
            (r * n_col + h * n_row + r, r * n_col + (1 - h) * n_row + r)
            for r in range(n_row)
            for h in range(2)
        ]
        full = join(x, lax.ppermute(x, BOTH, pairs), high, 1)
        half = full.shape[0] // 2
        full = full.reshape((2, half) + full.shape[1:])
        give = lax.dynamic_index_in_dim(full, 1 - low_bit[0], 0, keepdims=False)
        mine = lax.dynamic_index_in_dim(full, low_bit[0], 0, keepdims=False)
        pairs = [
            (r * n_col + h * n_row + r, r * n_col + h * n_row + (r ^ 1))
            for r in range(n_row)
            for h in range(2)
        ]
        got = lax.ppermute(give, BOTH, pairs)
        mine = jnp.where(low == p, mine, got)
        held = [0, 1]
        for b in range(1, row_bits):
            mask = 1 << b
            pairs = [
                (r * n_col + h * n_row + (r ^ d), r * n_col + h * n_row + (r ^ d ^ mask))
                for r in range(n_row)
                for h in range(2)
                for d in held
            ]
            got = lax.ppermute(mine, BOTH, pairs)
            mine = jnp.where(((p ^ low) & mask) != 0, got, mine)
            held = held + [d ^ mask for d in held]
        whole = double(mine, 0, low_bit[0], "col", 1)
        return whole.reshape(local_rows, panel)

    stored = matrix[0, :, 0, :]
    if panel_tiles % n_row == 0 and panel_tiles % n_col == 0:
        per_r, per_c = panel // n_row, panel // n_col
        piece = stored[:, per_c : 2 * per_c].T.reshape(per_c // TILE, TILE, local_rows)
        piece = double(piece, 1, high, "col", n_row)
        for b in range(row_bits - 1, -1, -1):
            piece = double(piece, 2 if b < row_bits - 1 else 2, low_bit[b], "col", 1 << b) if False else double(piece, 1 + (row_bits - b), low_bit[b], "col", 1 << b)
        next_r = piece.reshape(panel, local_rows).T
        piece = stored[per_r : 2 * per_r, :].reshape(per_r // TILE, TILE, local_cols)
        for i, b in enumerate(range(row_bits - 1, -1, -1)):
            piece = double(piece, 1 + i, row_bit[b], "row", 1 << b)
        next_c = piece.reshape(panel, local_cols).T
    else:
        pick_c = (col_global[:, None] == panel + span[None, :]).astype(jnp.float32)
        pick_r = (row_global[:, None] == panel + span[None, :]).astype(jnp.float32)
        next_r = lax.psum(mm(stored, pick_c), "col")
        next_c = lax.psum(mm_t(stored, pick_r), "row")

    below_r = (row_global >= panel)[:, None]
    below_c = (col_global >= panel)[:, None]
    sl_r = jnp.where(below_r, s_r, jnp.zeros_like(s_r))
    embed_r = (row_global[:, None] == panel + span[None, :]).astype(jnp.float32)
    embed_c = (col_global[:, None] == panel + span[None, :]).astype(jnp.float32)
    edge_tiles_r = max(1, 2 * panel_tiles // n_row)
    top_r = edge_tiles_r * TILE
    small = jnp.concatenate([mm_t(sl_r, sl_r), mm_t(embed_r[:top_r], s_r[:top_r])], axis=0)
    small = sum_over(small, "row", 2)
    gram, s_next = small[:panel], small[panel:]

    p_c = sum_over(mm_t(stored, sl_r, HIGH), "row", 2)
    p_r = along(p_c.reshape(tiles_c, TILE, panel))

    factor = jnp.linalg.cholesky(gram)
    inv = lower_solve(factor, jnp.eye(panel, dtype=jnp.float32))
    top = mm_nt(s_next, inv)
    inverse = invert_shifted(jnp.eye(panel, dtype=jnp.float32) - top)

    def refresh(x, index, fixed):
        width = min(x.shape[0], max(TILE, panel // (n_row if x.shape[0] == local_rows else n_col)))
        pick = (index[:width, None] == span[None, :]).astype(jnp.float32)
        under = (index[:width] < panel)[:, None]
        return jnp.concatenate([jnp.where(under, mm(pick, fixed), x[:width]), x[width:]], axis=0)

    p_c = refresh(p_c, col_global, gram)
    p_r = refresh(p_r, row_global, gram)
    next_c = refresh(next_c, col_global, s_next.T)
    next_r = refresh(next_r, row_global, s_next.T)
    sl_c = jnp.where(below_c, s_c, jnp.zeros_like(s_c))

    y_r = mm_nt(sl_r, inv, HIGH) - embed_r
    y_c = mm_nt(sl_c, inv, HIGH) - embed_c
    z_r = mm_nt(p_r, inv, HIGH) - next_r
    z_c = mm_nt(p_c, inv, HIGH) - next_c
    wmat = sum_over(mm_t(y_r, z_r), "row")
    core = mm_nt(mm(inverse, wmat), inverse)
    v_r = mm_nt(z_r, inverse, HIGH) - 0.5 * mm(y_r, core, HIGH)
    v_c = mm_nt(z_c, inverse, HIGH) - 0.5 * mm(y_c, core, HIGH)

    edge_r = max(TILE, panel // n_row)
    edge_c = min(128, local_cols)
    cols_pick = (span[:, None] == col_global[None, :edge_c]).astype(jnp.float32)
    rows_pick = (row_global[:edge_r, None] == span[None, :]).astype(jnp.float32)
    left = mm(s_r, cols_pick)
    in_c = (col_global < panel)[None, :]
    in_r = (row_global < panel)[:, None]
    edge_cols = jnp.where(in_c[:, :edge_c], left, stored[:, :edge_c])
    upper = mm_nt(rows_pick, s_c)
    left_top = jnp.concatenate(
        [left[:edge_r], jnp.zeros((edge_r, local_cols - edge_c), jnp.float32)], axis=1
    )
    edge_rows = jnp.where(
        in_r[:edge_r],
        jnp.where(in_c, 0.5 * (left_top + upper), upper),
        jnp.where(in_c, left_top, stored[:edge_r]),
    )
    return update(
        matrix,
        jnp.concatenate([y_r, v_r], axis=1),
        jnp.concatenate([v_c, y_c], axis=1),
        edge_rows,
        edge_cols,
    )


def solution(mesh):
    in_specs = (
        P(("row", "col"), None),
        P(("row", "col"), None),
        P(("row", "col")),
        P("row", None, "col", None),
    )
    out_specs = P("row", None, "col", None)
    return jax.shard_map(
        per_device, mesh=mesh, in_specs=in_specs, out_specs=out_specs, check_vma=False
    )
```

```python
import functools
import math

import jax
import jax.numpy as jnp
from jax import lax
from jax.experimental import pallas as pl
from jax.experimental.pallas import tpu as pltpu
from jax.sharding import PartitionSpec as P

TILE = 16
HIGH = lax.Precision.HIGH
HIGHEST = lax.Precision.HIGHEST
BOTH = ("row", "col")


def mm(a, b, precision=HIGHEST):
    return jnp.dot(a, b, precision=precision, preferred_element_type=jnp.float32)


def mm_t(a, b, precision=HIGHEST):
    return lax.dot_general(
        a, b, (((0,), (0,)), ((), ())), precision=precision, preferred_element_type=jnp.float32
    )


def mm_nt(a, b, precision=HIGHEST):
    return lax.dot_general(
        a, b, (((1,), (1,)), ((), ())), precision=precision, preferred_element_type=jnp.float32
    )


def swap(x, axis, mask):
    size = lax.axis_size(axis)
    return lax.ppermute(x, axis, [(i, i ^ mask) for i in range(size)])


def halve(addends, bit, axis, mask, sent=None):
    send = sum(lax.dynamic_index_in_dim(x, 1 - bit, 0, keepdims=False) for x in addends)
    keep = sum(lax.dynamic_index_in_dim(x, bit, 0, keepdims=False) for x in addends)
    if sent is not None:
        sent.append(send)
    return [keep, swap(send, axis, mask)]


def join(own, other, bit, dim):
    own, other = jnp.expand_dims(own, dim), jnp.expand_dims(other, dim)
    shape = own.shape[:dim] + (2,) + own.shape[dim + 1 :]
    return jnp.where(lax.broadcasted_iota(jnp.int32, shape, dim) == bit, own, other)


def double(x, dim, bit, axis, mask):
    return join(x, swap(x, axis, mask), bit, dim)


def sum_over(x, axis, streams=1):
    bits = int(math.log2(lax.axis_size(axis)))
    parts = jnp.split(x, streams, axis=0) if streams > 1 else [x]
    for step in range(bits):
        parts = [
            part + swap(part, axis, 1 << ((step + s) % bits)) for s, part in enumerate(parts)
        ]
    return jnp.concatenate(parts, axis=0) if streams > 1 else parts[0]


SUB = 8


def inverse_factor(a):
    n = a.shape[0]
    groups = [a[g * SUB : (g + 1) * SUB, :] for g in range(n // SUB)]
    lane = lax.broadcasted_iota(jnp.int32, (SUB, n), 1)
    sub = lax.broadcasted_iota(jnp.int32, (SUB, n), 0)

    def spread(x, k):
        return jnp.broadcast_to(x[:, k : k + 1], (SUB, n))

    out = []
    for k in range(0, n, SUB):
        own = groups[k // SUB]
        inside = (lane >= k) & (lane < k + SUB)
        rows = [jnp.broadcast_to(own[j : j + 1, :], (SUB, n)) for j in range(SUB)]
        pivots = [
            [spread(rows[j], k + c) if c >= j else None for c in range(SUB)] for j in range(SUB)
        ]
        rows = [jnp.where(inside, 0.0, x) for x in rows]
        recips = []
        done = jnp.zeros((SUB, n), jnp.float32)
        for j in range(SUB):
            recip = 1.0 / pivots[j][j]
            recips.append(recip)
            rows[j] = jnp.where(lane == k + j, 1.0, rows[j])
            for i in range(j + 1, SUB):
                m = pivots[j][i] * recip
                rows[i] = rows[i] - m * rows[j]
                for c in range(i, SUB):
                    pivots[i][c] = pivots[i][c] - m * pivots[j][c]
            done = jnp.where(sub == j, rows[j] * lax.rsqrt(pivots[j][j]), done)
        out.append(jnp.where(lane <= k + sub, done, 0.0))
        for g in range(k // SUB + 1, n // SUB):
            x = groups[g]
            cols = [spread(x, k + c) for c in range(SUB)]
            x = jnp.where(inside, 0.0, x)
            for j in range(SUB):
                f = cols[j] * recips[j]
                x = x - f * rows[j]
                for c in range(j + 1, SUB):
                    cols[c] = cols[c] - f * pivots[j][c]
            groups[g] = x
    return jnp.concatenate(out, axis=0)


def factor_kernel(gram_ref, inv_ref):
    inv_ref[...] = inverse_factor(gram_ref[...])


def shifted_kernel(inv_ref, next_ref, inverse_ref):
    n = inv_ref.shape[0]
    top = mm_nt(next_ref[...], inv_ref[...])
    r = lax.broadcasted_iota(jnp.int32, (n, n), 0)
    c = lax.broadcasted_iota(jnp.int32, (n, n), 1)
    shifted = jnp.where(r == c, 1.0, 0.0) - top
    second = inverse_factor(mm_t(shifted, shifted))
    inverse_ref[...] = mm_t(second, mm_nt(second, shifted))


def square_call(kernel, *operands):
    n = operands[0].shape[0]
    vmem = pl.BlockSpec(memory_space=pltpu.VMEM)
    return pl.pallas_call(
        kernel,
        out_shape=jax.ShapeDtypeStruct((n, n), jnp.float32),
        in_specs=[vmem] * len(operands),
        out_specs=vmem,
        compiler_params=pltpu.CompilerParams(vmem_limit_bytes=8 << 20),
        cost_estimate=pl.CostEstimate(flops=1 << 25, bytes_accessed=3 * n * n * 4, transcendentals=0),
    )(*operands)


def term_kernel(plan, bit_ref, count_ref, psi_ref, hpsi_ref, *rest_refs):
    rest, fold, n_row, sizes, orders = plan
    outs = rest_refs[: len(sizes)]
    buf, held, sem, held_sem = rest_refs[len(sizes) :]
    width = buf.shape[2]
    group = fold * n_row * TILE
    bit = bit_ref[0]

    step = max(1, 512 // group)
    while rest % step or any(size % step for size in sizes):
        step //= 2
    wide, steps = step * group, rest // step

    def load(i, j):
        at = pl.ds(pl.multiple_of((2 * i + bit) * width + j * wide, 128), wide)
        return pltpu.make_async_copy(
            psi_ref.at[:, at], buf.at[i, :, pl.ds(j * wide, wide)], sem.at[i * steps + j]
        )

    fetch = pltpu.make_async_copy(hpsi_ref, held, held_sem)
    fetch.start()
    for i in range(n_row // 2):
        for j in range(steps):
            load(i, j).start()
    fetch.wait()
    live = lax.broadcasted_iota(jnp.int32, held.shape, 0) < count_ref[0]
    hcols = jnp.where(live, held[...].astype(jnp.float32), 0.0).astype(jnp.bfloat16)
    for i in range(n_row // 2):
        for j in range(0, rest, step):
            load(i, j // step).wait()
            value = lax.dot_general(
                buf[i, :, j * group : (j + step) * group],
                hcols,
                (((0,), (0,)), ((), ())),
                preferred_element_type=jnp.float32,
            )
            value = value.reshape(step, fold * n_row, TILE, hcols.shape[1])
            stream, at = (0, j) if j < sizes[0] else (1, j - sizes[0])
            for h in range(fold):
                for r in range(n_row):
                    lead = tuple((r >> b) & 1 for b in orders[stream])
                    outs[stream][lead + (i, h, slice(at, at + step))] = value[:, h * n_row + r]


def s_term(bit, slab_counts, psi, hpsi, plan):
    rest, fold, n_row, sizes, orders = plan
    slots, bands = psi.shape
    panel = hpsi.shape[1]
    vmem = pl.BlockSpec(memory_space=pltpu.VMEM)
    smem = pl.BlockSpec(memory_space=pltpu.SMEM)
    lead = (2,) * len(orders[0]) + (n_row // 2, fold)
    return pl.pallas_call(
        lambda *refs: term_kernel(plan, *refs),
        out_shape=[jax.ShapeDtypeStruct(lead + (n, TILE, panel), jnp.float32) for n in sizes],
        in_specs=[smem, smem] + [pl.BlockSpec(memory_space=pltpu.HBM)] * 2,
        out_specs=[vmem] * len(sizes),
        scratch_shapes=[
            pltpu.VMEM((n_row // 2, slots, bands // n_row), jnp.bfloat16),
            pltpu.VMEM((slots, panel), jnp.bfloat16),
            pltpu.SemaphoreType.DMA((n_row // 2 * rest,)),
            pltpu.SemaphoreType.DMA,
        ],
        compiler_params=pltpu.CompilerParams(vmem_limit_bytes=58 << 20),
        cost_estimate=pl.CostEstimate(
            flops=slots * bands * panel, bytes_accessed=bands * (slots + 2 * panel), transcendentals=0
        ),
        name="s_term",
    )(bit, slab_counts, psi, hpsi)


def places_kernel(n_row, n_col, p_ref, q_ref, *outs):
    r0, r1, under_r, c0, c1, under_c, lane_c = outs
    panel = r0.shape[1]

    def index(ref, dim, parts, place):
        local = lax.broadcasted_iota(jnp.int32, ref.shape, dim)
        return (local // TILE * parts + place) * TILE + local % TILE

    def one_hot(ref, parts, place, base):
        k = lax.broadcasted_iota(jnp.int32, ref.shape, 1)
        ref[...] = jnp.where(index(ref, 0, parts, place) == base + k, 1.0, 0.0)

    p, q = p_ref[0], q_ref[0]
    one_hot(r0, n_row, p, 0)
    one_hot(r1, n_row, p, panel)
    one_hot(c0, n_col, q, 0)
    one_hot(c1, n_col, q, panel)
    under_r[...] = jnp.where(index(under_r, 0, n_row, p) < panel, 1.0, 0.0)
    under_c[...] = jnp.where(index(under_c, 0, n_col, q) < panel, 1.0, 0.0)
    lane_c[...] = jnp.where(index(lane_c, 1, n_col, q) < panel, 1.0, 0.0)


def places(n_row, n_col, p, q, panel, width_r, top_r, edge_c, width_c, top_c):
    smem = pl.BlockSpec(memory_space=pltpu.SMEM)
    vmem = pl.BlockSpec(memory_space=pltpu.VMEM)
    shapes = [(width_r, panel), (top_r, panel), (width_r, panel), (edge_c, panel), (top_c, panel)]
    shapes += [(width_c, panel), (SUB, edge_c)]
    return pl.pallas_call(
        functools.partial(places_kernel, n_row, n_col),
        out_shape=[jax.ShapeDtypeStruct(shape, jnp.float32) for shape in shapes],
        in_specs=[smem, smem],
        out_specs=[vmem] * len(shapes),
        compiler_params=pltpu.CompilerParams(vmem_limit_bytes=4 << 20),
        name="places",
    )(p.reshape(1), q.reshape(1))


def relay_kernel(blocks, m_ref, *refs):
    o_ref, buf, in_sem, out_sem = refs[-4:]
    rows = buf.shape[0] // blocks

    def load(i):
        at = pl.ds(i * rows, rows)
        return pltpu.make_async_copy(m_ref.at[0, at, 0, :], buf.at[at, :], in_sem.at[i])

    def store(i):
        at = pl.ds(i * rows, rows)
        return pltpu.make_async_copy(buf.at[at, :], o_ref.at[at, :], out_sem.at[i])

    for i in range(blocks):
        load(i).start()
    for i in range(blocks):
        load(i).wait()
        store(i).start()
    for i in range(blocks):
        store(i).wait()


def relay(matrix, after):
    rows, cols = matrix.shape[1], matrix.shape[3]
    blocks = max(1, rows // 256)
    hbm = pl.BlockSpec(memory_space=pltpu.HBM)
    return pl.pallas_call(
        functools.partial(relay_kernel, blocks),
        out_shape=jax.ShapeDtypeStruct((rows, cols), jnp.float32),
        in_specs=[hbm] + [pl.BlockSpec(memory_space=pl.ANY)] * len(after),
        out_specs=hbm,
        scratch_shapes=[
            pltpu.VMEM((rows, cols), jnp.float32),
            pltpu.SemaphoreType.DMA((blocks,)),
            pltpu.SemaphoreType.DMA((blocks,)),
        ],
        compiler_params=pltpu.CompilerParams(vmem_limit_bytes=50 << 20),
        cost_estimate=pl.CostEstimate(flops=1 << 22, bytes_accessed=8 * rows * cols, transcendentals=0),
        name="relay",
    )(matrix, *after)


def product_kernel(blocks, m_ref, s_ref, under_ref, r1_ref, o_ref, small_ref, sl_ref, total):
    rows = m_ref.shape[0] // blocks
    panel = s_ref.shape[1]
    width, top = under_ref.shape[0], r1_ref.shape[0]

    def tn(a, b):
        return lax.dot_general(a, b, (((0,), (0,)), ((), ())), preferred_element_type=jnp.float32)

    sl_ref[...] = s_ref[...]
    sl_ref[:width, :] = jnp.where(under_ref[...] > 0.5, 0.0, s_ref[:width, :])
    small_ref[:panel, :] = mm_t(sl_ref[...], sl_ref[...])
    small_ref[panel:, :] = mm_t(r1_ref[...], s_ref[:top, :])
    for i in range(blocks):
        at = pl.ds(i * rows, rows)
        s_high, s_low = split(sl_ref[at, :])
        m_high, m_low = split(m_ref[at, :])
        both = tn(jnp.concatenate([s_high, s_low], axis=1), m_high)
        term = both[:panel] + (both[panel:] + tn(s_high, m_low))
        total[...] = term if i == 0 else total[...] + term
    o_ref[...] = total[...].T


def product(stored, s, under, r1):
    (rows, cols), panel = stored.shape, s.shape[1]
    blocks = max(1, rows // 256)
    vmem = pl.BlockSpec(memory_space=pltpu.VMEM)
    return pl.pallas_call(
        functools.partial(product_kernel, blocks),
        out_shape=[
            jax.ShapeDtypeStruct((cols, panel), jnp.float32),
            jax.ShapeDtypeStruct((2 * panel, panel), jnp.float32),
            jax.ShapeDtypeStruct((rows, panel), jnp.float32),
        ],
        in_specs=[vmem] * 4,
        out_specs=[vmem] * 3,
        scratch_shapes=[pltpu.VMEM((panel, cols), jnp.float32)],
        compiler_params=pltpu.CompilerParams(vmem_limit_bytes=24 << 20),
        cost_estimate=pl.CostEstimate(
            flops=6 * rows * cols * panel, bytes_accessed=4 * rows * cols, transcendentals=0
        ),
        name="product",
    )(stored, s, under, r1)


def split(x):
    high = x.astype(jnp.bfloat16)
    return high, (x - high.astype(jnp.float32)).astype(jnp.bfloat16)


def nt(a, b):
    return lax.dot_general(a, b, (((1,), (1,)), ((), ())), preferred_element_type=jnp.float32)


def update_kernel(
    blocks, m_ref, y_ref, p_ref, r_ref, under_ref, fix_ref, r1_ref, core_ref, x_ref, right_ref,
    edge_rows_ref, edge_cols_ref, o_ref, buf, out_sem,
):
    rows = buf.shape[0] // blocks
    edge_r = edge_rows_ref.shape[0]
    edge_c = edge_cols_ref.shape[1]

    def store(i):
        at = pl.ds(i * rows, rows)
        return pltpu.make_async_copy(buf.at[at, :], o_ref.at[0, at, 0, :], out_sem.at[i])

    right_high, right_low = split(right_ref[...])
    right = jnp.concatenate([right_high, right_low, right_high], axis=1)
    x_high, x_low = split(x_ref[...])
    x = jnp.concatenate([x_high, x_low, x_high], axis=0)
    for i in range(blocks):
        at = pl.ds(i * rows, rows)
        p = p_ref[at, :]
        if i == 0:
            top = jnp.where(under_ref[...] > 0.5, fix_ref[...], p[:edge_r])
            p = jnp.concatenate([top, p[edge_r:]], axis=0)
        p_high, p_low = split(p)
        v = jnp.dot(
            jnp.concatenate([p_high, p_high, p_low], axis=1), x, preferred_element_type=jnp.float32
        )
        v = v - r_ref[at, :]
        y = y_ref[at, :]
        if i == 0:
            n = r1_ref.shape[0]
            v = jnp.concatenate([v[:n] + mm(r1_ref[...], core_ref[...]), v[n:]], axis=0)
            y = jnp.concatenate([y[:n] - r1_ref[...], y[n:]], axis=0)
        left_high, left_low = split(jnp.concatenate([y, v], axis=1))
        term = nt(jnp.concatenate([left_high, left_high, left_low], axis=1), right)
        buf[at, :edge_c] = edge_cols_ref[at, :] - term[:, :edge_c]
        if edge_c < buf.shape[1]:
            buf[at, edge_c:] = m_ref[at, edge_c:] - term[:, edge_c:]
        if i == 0:
            buf[:edge_r, :] = edge_rows_ref[...] - term[:edge_r]
        store(i).start()
    for i in range(blocks):
        store(i).wait()


def update(shape, stored, *operands):
    rows, cols = stored.shape
    blocks = max(1, rows // 256)
    vmem = pl.BlockSpec(memory_space=pltpu.VMEM)
    return pl.pallas_call(
        functools.partial(update_kernel, blocks),
        out_shape=jax.ShapeDtypeStruct(shape, jnp.float32),
        in_specs=[vmem] * (1 + len(operands)),
        out_specs=pl.BlockSpec(memory_space=pltpu.HBM),
        scratch_shapes=[
            pltpu.VMEM((rows, cols), jnp.float32),
            pltpu.SemaphoreType.DMA((blocks,)),
        ],
        compiler_params=pltpu.CompilerParams(vmem_limit_bytes=28 << 20),
        cost_estimate=pl.CostEstimate(
            flops=6 * rows * cols * 256, bytes_accessed=8 * rows * cols, transcendentals=0
        ),
        name="update",
    )(stored, *operands)


def step_of(psi, hpsi, slab_counts, matrix):
    p = lax.axis_index("row")
    q = lax.axis_index("col")
    n_row = lax.axis_size("row")
    n_col = lax.axis_size("col")
    fold = n_col // n_row
    if n_col % n_row or fold != 2 or n_row & (n_row - 1) or n_row < 2:
        raise ValueError("mesh shape")
    low, high = q % n_row, q // n_row
    panel = hpsi.shape[1]
    local_rows, local_cols = matrix.shape[1], matrix.shape[3]
    tiles_c = local_cols // TILE
    row_bits = int(math.log2(n_row))
    panel_tiles = panel // TILE

    width_r, width_c = max(TILE, panel // n_row), max(TILE, panel // n_col)
    top_r = max(1, 2 * panel_tiles // n_row) * TILE
    top_c = max(1, 2 * panel_tiles // n_col) * TILE
    edge_c = min(128, local_cols)
    if max(width_r, top_r) > local_rows or max(width_c, top_c) > edge_c:
        raise ValueError("block size")

    rest = tiles_c // n_row
    low_bit = [(low >> i) & 1 for i in range(row_bits)]
    row_bit = [(p >> i) & 1 for i in range(row_bits)]
    streams = 2 if rest % 2 == 0 else 1
    orders = [[(i + k) % row_bits for i in range(row_bits)] for k in range(streams)]
    plan = (rest, fold, n_row, [rest // streams] * streams, orders)
    theirs = s_term((1 - low_bit[0]).reshape(1), slab_counts, psi, hpsi, plan)
    got = [swap(x, "col", 1) for x in theirs]
    r0, r1, under_r, c0, c1, under_c, lane_c = places(
        n_row, n_col, p, q, panel, width_r, top_r, edge_c, width_c, top_c
    )
    mine = s_term(low_bit[0].reshape(1), slab_counts, psi, hpsi, plan)
    parts = [list(pair) for pair in zip(mine, got)]
    sent = []
    for step in range(row_bits):
        for k in range(streams):
            b = orders[k][step]
            parts[k] = halve(parts[k], row_bit[b], "row", 1 << b, sent)
    s = [jnp.concatenate([part[i] for part in parts], axis=2) for i in range(2)]
    s = [x.reshape((2,) * (row_bits - 1) + x.shape[1:]) for x in s]
    for b in range(row_bits - 1, 0, -1):
        s = halve(s, low_bit[b], "col", 1 << b)
    s = sum(halve(s, high, "col", n_row))
    s = double(s, 0, high, "col", n_row)
    for b in range(row_bits - 1, -1, -1):
        s = double(s, 0, low_bit[b], "col", 1 << b)
    s = s.transpose(tuple(range(row_bits - 1, -1, -1)) + (row_bits + 1, row_bits) + (row_bits + 2, row_bits + 3))
    s = s.reshape(tiles_c, fold, TILE, panel)
    s_r = s.reshape(local_rows, panel)
    own_cols = lax.dynamic_index_in_dim(s, high, 1, keepdims=False)

    def across(x, step):
        mask = 1 << step
        pairs = [
            ((c % n_row ^ d) * n_col + c, (c % n_row ^ d ^ mask) * n_col + c)
            for c in range(n_col)
            for d in range(mask)
        ]
        other = lax.ppermute(x, BOTH, pairs)
        return jnp.where(((p ^ low) & mask) != 0, other, x)

    def along(x, before):
        pairs = [
            (r * n_col + h * n_row + r, r * n_col + (1 - h) * n_row + r)
            for r in range(n_row)
            for h in range(2)
        ]
        other = lax.ppermute(x, BOTH, pairs)
        full = join(x, other, high, 1)
        half = full.shape[0] // 2
        full = full.reshape((2, half) + full.shape[1:])
        give = lax.dynamic_index_in_dim(full, 1 - low_bit[0], 0, keepdims=False)
        mine = lax.dynamic_index_in_dim(full, low_bit[0], 0, keepdims=False)
        pairs = [
            (r * n_col + h * n_row + r, r * n_col + h * n_row + (r ^ 1))
            for r in range(n_row)
            for h in range(2)
        ]
        (give, mine), _ = lax.optimization_barrier(((give, mine), before))
        got = lax.ppermute(give, BOTH, pairs)
        mine = jnp.where(low == p, mine, got)
        first = mine
        held = [0, 1]
        for b in range(1, row_bits):
            mask = 1 << b
            pairs = [
                (r * n_col + h * n_row + (r ^ d), r * n_col + h * n_row + (r ^ d ^ mask))
                for r in range(n_row)
                for h in range(2)
                for d in held
            ]
            got = lax.ppermute(mine, BOTH, pairs)
            mine = jnp.where(((p ^ low) & mask) != 0, got, mine)
            held = held + [d ^ mask for d in held]
        whole = double(mine, 0, low_bit[0], "col", 1)
        return whole.reshape(local_rows, panel), first

    stored = relay(matrix, sent[:streams])
    lead_rows, lead_cols = stored[:top_r], stored[:, :edge_c]
    if panel_tiles % n_row == 0 and panel_tiles % n_col == 0:
        per_r, per_c = panel // n_row, panel // n_col
        piece = lead_cols[:, per_c : 2 * per_c].T.reshape(per_c // TILE, TILE, local_rows)
        piece = double(piece, 1, high, "col", n_row)
        for b in range(row_bits - 1, -1, -1):
            piece = double(piece, 1 + row_bits - b, low_bit[b], "col", 1 << b)
        next_rt = piece.reshape(panel, local_rows)
        piece = lead_rows[per_r : 2 * per_r, :].reshape(per_r // TILE, TILE, local_cols)
        for i, b in enumerate(range(row_bits - 1, -1, -1)):
            piece = double(piece, 1 + i, row_bit[b], "row", 1 << b)
        next_ct = piece.reshape(panel, local_cols)
    else:
        next_rt = lax.psum(mm(lead_cols[:, :top_c], c1), "col").T
        next_ct = lax.psum(mm_t(r1, lead_rows), "row")

    p_c, small, sl_r = product(stored, s_r, under_r, r1)
    small = sum_over(small, "row", 2)
    halves = list(jnp.split(p_c, 2, axis=0))
    for step in range(row_bits):
        if step == row_bits - 1:
            small, halves = lax.optimization_barrier((small, halves))
        halves = [
            half + swap(half, "row", 1 << ((step + k) % row_bits)) for k, half in enumerate(halves)
        ]
    gram, s_next = small[:panel], small[panel:]
    inv = square_call(factor_kernel, gram)
    inverse = square_call(shifted_kernel, inv, s_next)
    halves, inv, inverse = lax.optimization_barrier((halves, inv, inverse))
    p_c = jnp.concatenate(halves, axis=0)

    def top_set(x, under, fixed):
        width = under.shape[0]
        return x.at[:width].set(jnp.where(under > 0.5, fixed, x[:width]))

    def less(x, one_hot):
        return x.at[: one_hot.shape[0]].add(-one_hot)

    z_c = mm_nt(p_c, inv, HIGH) - next_ct.T
    z_c = top_set(z_c, under_c, mm_nt(mm(c0[:width_c], gram), inv) - mm_nt(c0[:width_c], s_next))
    s_own = top_set(own_cols.reshape(local_cols, panel), under_c, 0.0)
    y_own = less(mm_nt(s_own, inv, HIGH), c1)
    s_c, y_own, _ = lax.optimization_barrier((own_cols, y_own, p_c))
    wmat = jnp.where(p == low, mm_t(y_own, z_c), 0.0)
    p_r, passed = along(p_c.reshape(tiles_c, TILE, panel), wmat)
    for step in range(row_bits):
        wmat = wmat + swap(wmat, "row", 1 << step)
    wmat, _ = lax.optimization_barrier((wmat, passed))
    wmat = wmat + swap(wmat, "col", 1)
    wmat = wmat + swap(wmat, "col", n_row)
    for b in range(1, row_bits):
        wmat = wmat + swap(wmat, "col", 1 << b)

    for step in range(row_bits):
        s_c = across(s_c, step)
    s_c = s_c.reshape(local_cols, panel)
    y_c = less(mm_nt(top_set(s_c, under_c, 0.0), inv, HIGH), c1)

    half_core = 0.5 * mm_nt(mm(inverse, wmat), inverse)
    v_c = mm_nt(z_c, inverse, HIGH) - mm(y_c, half_core, HIGH)
    y_r = mm_nt(sl_r, inv, HIGH)
    r_r = mm_t(next_rt, inverse.T, HIGH) + mm(y_r, half_core, HIGH)
    r_r = top_set(r_r, under_r, mm_nt(mm_nt(r0, s_next), inverse))

    left = mm_nt(s_r, c0)
    edge_cols = jnp.where(lane_c[:1] > 0.5, left, lead_cols)
    upper = mm_nt(r0, s_c)
    in_r = under_r[:, :1] > 0.5
    corner = jnp.where(
        in_r,
        jnp.where(lane_c[:1] > 0.5, 0.5 * (left[:width_r] + upper[:, :edge_c]), upper[:, :edge_c]),
        edge_cols[:width_r],
    )
    edge_rows = jnp.concatenate(
        [corner, jnp.where(in_r, upper[:, edge_c:], lead_rows[:width_r, edge_c:])], axis=1
    )
    return update(
        matrix.shape,
        stored,
        y_r,
        p_r,
        r_r,
        under_r,
        mm(r0, gram),
        r1,
        half_core,
        mm_t(inv, inverse.T),
        jnp.concatenate([v_c, y_c], axis=1),
        edge_rows,
        edge_cols,
    )


def solution(mesh):
    in_specs = (
        P(("row", "col"), None),
        P(("row", "col"), None),
        P(("row", "col")),
        P("row", None, "col", None),
    )
    out_specs = P("row", None, "col", None)
    return jax.shard_map(
        step_of, mesh=mesh, in_specs=in_specs, out_specs=out_specs, check_vma=False
    )
```

```python
import functools
import math

import jax
import jax.numpy as jnp
from jax import lax
from jax.experimental import pallas as pl
from jax.experimental.pallas import tpu as pltpu
from jax.sharding import PartitionSpec as P

TILE = 16
HIGH = lax.Precision.HIGH
HIGHEST = lax.Precision.HIGHEST
BOTH = ("row", "col")


def mm(a, b, precision=HIGHEST):
    return jnp.dot(a, b, precision=precision, preferred_element_type=jnp.float32)


def mm_t(a, b, precision=HIGHEST):
    return lax.dot_general(
        a, b, (((0,), (0,)), ((), ())), precision=precision, preferred_element_type=jnp.float32
    )


def mm_nt(a, b, precision=HIGHEST):
    return lax.dot_general(
        a, b, (((1,), (1,)), ((), ())), precision=precision, preferred_element_type=jnp.float32
    )


def swap(x, axis, mask):
    size = lax.axis_size(axis)
    return lax.ppermute(x, axis, [(i, i ^ mask) for i in range(size)])


def halve(addends, bit, axis, mask, sent=None):
    send = sum(lax.dynamic_index_in_dim(x, 1 - bit, 0, keepdims=False) for x in addends)
    keep = sum(lax.dynamic_index_in_dim(x, bit, 0, keepdims=False) for x in addends)
    if sent is not None:
        sent.append(send)
    return [keep, swap(send, axis, mask)]


def join(own, other, bit, dim):
    own, other = jnp.expand_dims(own, dim), jnp.expand_dims(other, dim)
    shape = own.shape[:dim] + (2,) + own.shape[dim + 1 :]
    return jnp.where(lax.broadcasted_iota(jnp.int32, shape, dim) == bit, own, other)


def double(x, dim, bit, axis, mask):
    return join(x, swap(x, axis, mask), bit, dim)


def sum_masks(x, axis, masks):
    if len(masks) != 2:
        for mask in masks:
            x = x + swap(x, axis, mask)
        return x
    first, second = masks
    near, far, both = (swap(x, axis, mask) for mask in (first, second, first ^ second))
    return (x + near) + (far + both)


def sum_over(x, axis, streams=1):
    bits = int(math.log2(lax.axis_size(axis)))
    parts = jnp.split(x, streams, axis=0) if streams > 1 else [x]
    for step in range(bits):
        parts = [
            part + swap(part, axis, 1 << ((step + s) % bits)) for s, part in enumerate(parts)
        ]
    return jnp.concatenate(parts, axis=0) if streams > 1 else parts[0]


SUB = 8


def inverse_factor(a):
    n = a.shape[0]
    groups = [a[g * SUB : (g + 1) * SUB, :] for g in range(n // SUB)]
    lane = lax.broadcasted_iota(jnp.int32, (SUB, n), 1)
    sub = lax.broadcasted_iota(jnp.int32, (SUB, n), 0)

    def spread(x, k):
        return jnp.broadcast_to(x[:, k : k + 1], (SUB, n))

    out = []
    for k in range(0, n, SUB):
        own = groups[k // SUB]
        inside = (lane >= k) & (lane < k + SUB)
        rows = [jnp.broadcast_to(own[j : j + 1, :], (SUB, n)) for j in range(SUB)]
        pivots = [
            [spread(rows[j], k + c) if c >= j else None for c in range(SUB)] for j in range(SUB)
        ]
        rows = [jnp.where(inside, 0.0, x) for x in rows]
        recips = []
        done = jnp.zeros((SUB, n), jnp.float32)
        for j in range(SUB):
            recip = 1.0 / pivots[j][j]
            recips.append(recip)
            rows[j] = jnp.where(lane == k + j, 1.0, rows[j])
            for i in range(j + 1, SUB):
                m = pivots[j][i] * recip
                rows[i] = rows[i] - m * rows[j]
                for c in range(i, SUB):
                    pivots[i][c] = pivots[i][c] - m * pivots[j][c]
            done = jnp.where(sub == j, rows[j] * lax.rsqrt(pivots[j][j]), done)
        out.append(jnp.where(lane <= k + sub, done, 0.0))
        for g in range(k // SUB + 1, n // SUB):
            x = groups[g]
            cols = [spread(x, k + c) for c in range(SUB)]
            x = jnp.where(inside, 0.0, x)
            for j in range(SUB):
                f = cols[j] * recips[j]
                x = x - f * rows[j]
                for c in range(j + 1, SUB):
                    cols[c] = cols[c] - f * pivots[j][c]
            groups[g] = x
    return jnp.concatenate(out, axis=0)


def factor_kernel(gram_ref, inv_ref):
    inv_ref[...] = inverse_factor(gram_ref[...])


def shifted_kernel(inv_ref, next_ref, inverse_ref):
    n = inv_ref.shape[0]
    top = mm_nt(next_ref[...], inv_ref[...])
    r = lax.broadcasted_iota(jnp.int32, (n, n), 0)
    c = lax.broadcasted_iota(jnp.int32, (n, n), 1)
    shifted = jnp.where(r == c, 1.0, 0.0) - top
    second = inverse_factor(mm_t(shifted, shifted))
    inverse_ref[...] = mm_t(second, mm_nt(second, shifted))


def square_call(kernel, *operands):
    n = operands[0].shape[0]
    vmem = pl.BlockSpec(memory_space=pltpu.VMEM)
    return pl.pallas_call(
        kernel,
        out_shape=jax.ShapeDtypeStruct((n, n), jnp.float32),
        in_specs=[vmem] * len(operands),
        out_specs=vmem,
        compiler_params=pltpu.CompilerParams(vmem_limit_bytes=8 << 20),
        cost_estimate=pl.CostEstimate(flops=1 << 25, bytes_accessed=3 * n * n * 4, transcendentals=0),
    )(*operands)


def term_kernel(plan, bit_ref, count_ref, psi_ref, hpsi_ref, *rest_refs):
    rest, fold, n_row, sizes, orders = plan
    outs = rest_refs[: 2 * len(sizes)]
    buf, held, sem, held_sem = rest_refs[2 * len(sizes) :]
    width = buf.shape[2]
    group = fold * n_row * TILE
    bit = bit_ref[0]
    step = max(1, 512 // group)
    while rest % step or any(size % step for size in sizes):
        step //= 2

    def load(which, i):
        at = pl.ds(pl.multiple_of((2 * i + (1 - bit if which else bit)) * width, 128), width)
        slot = which * (n_row // 2) + i
        return pltpu.make_async_copy(psi_ref.at[:, at], buf.at[slot], sem.at[slot])

    fetch = pltpu.make_async_copy(hpsi_ref, held, held_sem)
    fetch.start()
    for which in range(2):
        for i in range(n_row // 2):
            load(which, i).start()
    fetch.wait()
    live = lax.broadcasted_iota(jnp.int32, held.shape, 0) < count_ref[0]
    hcols = jnp.where(live, held[...].astype(jnp.float32), 0.0).astype(jnp.bfloat16)
    for which in range(2):
        for i in range(n_row // 2):
            load(which, i).wait()
            for j in range(0, rest, step):
                value = lax.dot_general(
                    buf[which * (n_row // 2) + i, :, j * group : (j + step) * group],
                    hcols,
                    (((0,), (0,)), ((), ())),
                    preferred_element_type=jnp.float32,
                )
                value = value.reshape(step, fold * n_row, TILE, hcols.shape[1])
                stream, at = (0, j) if j < sizes[0] else (1, j - sizes[0])
                out = outs[which * len(sizes) + stream]
                for h in range(fold):
                    for r in range(n_row):
                        lead = tuple((r >> b) & 1 for b in orders[stream])
                        out[lead + (i, h, slice(at, at + step))] = value[:, h * n_row + r]


def s_term(bit, slab_counts, psi, hpsi, plan):
    _, fold, n_row, sizes, orders = plan
    slots, bands = psi.shape
    panel = hpsi.shape[1]
    vmem = pl.BlockSpec(memory_space=pltpu.VMEM)
    smem = pl.BlockSpec(memory_space=pltpu.SMEM)
    lead = (2,) * len(orders[0]) + (n_row // 2, fold)
    out = pl.pallas_call(
        lambda *refs: term_kernel(plan, *refs),
        out_shape=[jax.ShapeDtypeStruct(lead + (n, TILE, panel), jnp.float32) for n in sizes * 2],
        in_specs=[smem, smem] + [pl.BlockSpec(memory_space=pltpu.HBM)] * 2,
        out_specs=[vmem] * (2 * len(sizes)),
        scratch_shapes=[
            pltpu.VMEM((n_row, slots, bands // n_row), jnp.bfloat16),
            pltpu.VMEM((slots, panel), jnp.bfloat16),
            pltpu.SemaphoreType.DMA((n_row,)),
            pltpu.SemaphoreType.DMA,
        ],
        compiler_params=pltpu.CompilerParams(vmem_limit_bytes=56 << 20),
        cost_estimate=pl.CostEstimate(
            flops=2 * slots * bands * panel, bytes_accessed=2 * bands * (slots + 2 * panel), transcendentals=0
        ),
        name="s_term",
    )(bit, slab_counts, psi, hpsi)
    return out[: len(sizes)], out[len(sizes) :]


def places_kernel(n_row, n_col, p_ref, q_ref, *outs):
    r0, r1, under_r, c0, c1, under_c, lane_c = outs
    panel = r0.shape[1]

    def index(ref, dim, parts, place):
        local = lax.broadcasted_iota(jnp.int32, ref.shape, dim)
        return (local // TILE * parts + place) * TILE + local % TILE

    def one_hot(ref, parts, place, base):
        k = lax.broadcasted_iota(jnp.int32, ref.shape, 1)
        ref[...] = jnp.where(index(ref, 0, parts, place) == base + k, 1.0, 0.0)

    p, q = p_ref[0], q_ref[0]
    one_hot(r0, n_row, p, 0)
    one_hot(r1, n_row, p, panel)
    one_hot(c0, n_col, q, 0)
    one_hot(c1, n_col, q, panel)
    under_r[...] = jnp.where(index(under_r, 0, n_row, p) < panel, 1.0, 0.0)
    under_c[...] = jnp.where(index(under_c, 0, n_col, q) < panel, 1.0, 0.0)
    lane_c[...] = jnp.where(index(lane_c, 1, n_col, q) < panel, 1.0, 0.0)


def places(n_row, n_col, p, q, panel, width_r, top_r, edge_c, width_c, top_c):
    smem = pl.BlockSpec(memory_space=pltpu.SMEM)
    vmem = pl.BlockSpec(memory_space=pltpu.VMEM)
    shapes = [(width_r, panel), (top_r, panel), (width_r, panel), (edge_c, panel), (top_c, panel)]
    shapes += [(width_c, panel), (SUB, edge_c)]
    return pl.pallas_call(
        functools.partial(places_kernel, n_row, n_col),
        out_shape=[jax.ShapeDtypeStruct(shape, jnp.float32) for shape in shapes],
        in_specs=[smem, smem],
        out_specs=[vmem] * len(shapes),
        compiler_params=pltpu.CompilerParams(vmem_limit_bytes=4 << 20),
        name="places",
    )(p.reshape(1), q.reshape(1))


def relay_kernel(blocks, m_ref, *refs):
    o_ref, buf, in_sem, out_sem = refs[-4:]
    rows = buf.shape[0] // blocks

    def load(i):
        at = pl.ds(i * rows, rows)
        return pltpu.make_async_copy(m_ref.at[0, at, 0, :], buf.at[at, :], in_sem.at[i])

    def store(i):
        at = pl.ds(i * rows, rows)
        return pltpu.make_async_copy(buf.at[at, :], o_ref.at[at, :], out_sem.at[i])

    for i in range(blocks):
        load(i).start()
    for i in range(blocks):
        load(i).wait()
        store(i).start()
    for i in range(blocks):
        store(i).wait()


def relay(matrix, after):
    rows, cols = matrix.shape[1], matrix.shape[3]
    blocks = max(1, rows // 256)
    hbm = pl.BlockSpec(memory_space=pltpu.HBM)
    return pl.pallas_call(
        functools.partial(relay_kernel, blocks),
        out_shape=jax.ShapeDtypeStruct((rows, cols), jnp.float32),
        in_specs=[hbm] + [pl.BlockSpec(memory_space=pl.ANY)] * len(after),
        out_specs=hbm,
        scratch_shapes=[
            pltpu.VMEM((rows, cols), jnp.float32),
            pltpu.SemaphoreType.DMA((blocks,)),
            pltpu.SemaphoreType.DMA((blocks,)),
        ],
        compiler_params=pltpu.CompilerParams(vmem_limit_bytes=50 << 20),
        cost_estimate=pl.CostEstimate(flops=1 << 22, bytes_accessed=8 * rows * cols, transcendentals=0),
        name="relay",
    )(matrix, *after)


def product_kernel(blocks, m_ref, s_ref, under_ref, r1_ref, o_ref, small_ref, sl_ref, total):
    rows = m_ref.shape[0] // blocks
    panel = s_ref.shape[1]
    width, top = under_ref.shape[0], r1_ref.shape[0]

    def tn(a, b):
        return lax.dot_general(a, b, (((0,), (0,)), ((), ())), preferred_element_type=jnp.float32)

    sl_ref[...] = s_ref[...]
    sl_ref[:width, :] = jnp.where(under_ref[...] > 0.5, 0.0, s_ref[:width, :])
    small_ref[:panel, :] = mm_t(sl_ref[...], sl_ref[...])
    small_ref[panel:, :] = mm_t(r1_ref[...], s_ref[:top, :])
    for i in range(blocks):
        at = pl.ds(i * rows, rows)
        s_high, s_low = split(sl_ref[at, :])
        m_high, m_low = split(m_ref[at, :])
        both = tn(jnp.concatenate([s_high, s_low], axis=1), m_high)
        term = both[:panel] + (both[panel:] + tn(s_high, m_low))
        total[...] = term if i == 0 else total[...] + term
    o_ref[...] = total[...].T


def product(stored, s, under, r1):
    (rows, cols), panel = stored.shape, s.shape[1]
    blocks = max(1, rows // 256)
    vmem = pl.BlockSpec(memory_space=pltpu.VMEM)
    return pl.pallas_call(
        functools.partial(product_kernel, blocks),
        out_shape=[
            jax.ShapeDtypeStruct((cols, panel), jnp.float32),
            jax.ShapeDtypeStruct((2 * panel, panel), jnp.float32),
            jax.ShapeDtypeStruct((rows, panel), jnp.float32),
        ],
        in_specs=[vmem] * 4,
        out_specs=[vmem] * 3,
        scratch_shapes=[pltpu.VMEM((panel, cols), jnp.float32)],
        compiler_params=pltpu.CompilerParams(vmem_limit_bytes=24 << 20),
        cost_estimate=pl.CostEstimate(
            flops=6 * rows * cols * panel, bytes_accessed=4 * rows * cols, transcendentals=0
        ),
        name="product",
    )(stored, s, under, r1)


def split(x):
    high = x.astype(jnp.bfloat16)
    return high, (x - high.astype(jnp.float32)).astype(jnp.bfloat16)


def nt(a, b):
    return lax.dot_general(a, b, (((1,), (1,)), ((), ())), preferred_element_type=jnp.float32)


def update_kernel(
    blocks, m_ref, y_ref, p_ref, r_ref, under_ref, fix_ref, r1_ref, core_ref, x_ref, right_ref,
    edge_rows_ref, edge_cols_ref, o_ref, buf, out_sem,
):
    rows = buf.shape[0] // blocks
    edge_r = edge_rows_ref.shape[0]
    edge_c = edge_cols_ref.shape[1]

    def store(i):
        at = pl.ds(i * rows, rows)
        return pltpu.make_async_copy(buf.at[at, :], o_ref.at[0, at, 0, :], out_sem.at[i])

    right_high, right_low = split(right_ref[...])
    right = jnp.concatenate([right_high, right_low, right_high], axis=1)
    x_high, x_low = split(x_ref[...])
    x = jnp.concatenate([x_high, x_low, x_high], axis=0)
    for i in range(blocks):
        at = pl.ds(i * rows, rows)
        p = p_ref[at, :]
        if i == 0:
            top = jnp.where(under_ref[...] > 0.5, fix_ref[...], p[:edge_r])
            p = jnp.concatenate([top, p[edge_r:]], axis=0)
        p_high, p_low = split(p)
        v = jnp.dot(
            jnp.concatenate([p_high, p_high, p_low], axis=1), x, preferred_element_type=jnp.float32
        )
        v = v - r_ref[at, :]
        y = y_ref[at, :]
        if i == 0:
            n = r1_ref.shape[0]
            v = jnp.concatenate([v[:n] + mm(r1_ref[...], core_ref[...]), v[n:]], axis=0)
            y = jnp.concatenate([y[:n] - r1_ref[...], y[n:]], axis=0)
        left_high, left_low = split(jnp.concatenate([y, v], axis=1))
        term = nt(jnp.concatenate([left_high, left_high, left_low], axis=1), right)
        buf[at, :edge_c] = edge_cols_ref[at, :] - term[:, :edge_c]
        if edge_c < buf.shape[1]:
            buf[at, edge_c:] = m_ref[at, edge_c:] - term[:, edge_c:]
        if i == 0:
            buf[:edge_r, :] = edge_rows_ref[...] - term[:edge_r]
        store(i).start()
    for i in range(blocks):
        store(i).wait()


def update(shape, stored, *operands):
    rows, cols = stored.shape
    blocks = max(1, rows // 256)
    vmem = pl.BlockSpec(memory_space=pltpu.VMEM)
    return pl.pallas_call(
        functools.partial(update_kernel, blocks),
        out_shape=jax.ShapeDtypeStruct(shape, jnp.float32),
        in_specs=[vmem] * (1 + len(operands)),
        out_specs=pl.BlockSpec(memory_space=pltpu.HBM),
        scratch_shapes=[
            pltpu.VMEM((rows, cols), jnp.float32),
            pltpu.SemaphoreType.DMA((blocks,)),
        ],
        compiler_params=pltpu.CompilerParams(vmem_limit_bytes=28 << 20),
        cost_estimate=pl.CostEstimate(
            flops=6 * rows * cols * 256, bytes_accessed=8 * rows * cols, transcendentals=0
        ),
        name="update",
    )(stored, *operands)


def step_of(psi, hpsi, slab_counts, matrix):
    p = lax.axis_index("row")
    q = lax.axis_index("col")
    n_row = lax.axis_size("row")
    n_col = lax.axis_size("col")
    fold = n_col // n_row
    if n_col % n_row or fold != 2 or n_row & (n_row - 1) or n_row < 2:
        raise ValueError("mesh shape")
    low, high = q % n_row, q // n_row
    panel = hpsi.shape[1]
    local_rows, local_cols = matrix.shape[1], matrix.shape[3]
    tiles_c = local_cols // TILE
    row_bits = int(math.log2(n_row))
    panel_tiles = panel // TILE

    width_r, width_c = max(TILE, panel // n_row), max(TILE, panel // n_col)
    top_r = max(1, 2 * panel_tiles // n_row) * TILE
    top_c = max(1, 2 * panel_tiles // n_col) * TILE
    edge_c = min(128, local_cols)
    if max(width_r, top_r) > local_rows or max(width_c, top_c) > edge_c:
        raise ValueError("block size")

    rest = tiles_c // n_row
    low_bit = [(low >> i) & 1 for i in range(row_bits)]
    row_bit = [(p >> i) & 1 for i in range(row_bits)]
    streams = 2 if rest % 2 == 0 else 1
    orders = [[(i + k) % row_bits for i in range(row_bits)] for k in range(streams)]
    plan = (rest, fold, n_row, [rest // streams] * streams, orders)
    theirs, mine = s_term((1 - low_bit[0]).reshape(1), slab_counts, psi, hpsi, plan)
    got = [swap(x, "col", 1) for x in theirs]
    r0, r1, under_r, c0, c1, under_c, lane_c = places(
        n_row, n_col, p, q, panel, width_r, top_r, edge_c, width_c, top_c
    )
    parts = [list(pair) for pair in zip(mine, got)]
    sent = []
    for step in range(row_bits):
        for k in range(streams):
            b = orders[k][step]
            parts[k] = halve(parts[k], row_bit[b], "row", 1 << b, sent)
    s = [jnp.concatenate([part[i] for part in parts], axis=2) for i in range(2)]
    s = [x.reshape((2,) * (row_bits - 1) + x.shape[1:]) for x in s]
    for b in range(row_bits - 1, 0, -1):
        s = halve(s, low_bit[b], "col", 1 << b)
    s = sum(halve(s, high, "col", n_row))
    s = double(s, 0, high, "col", n_row)
    for b in range(row_bits - 1, 0, -1):
        s = double(s, 0, low_bit[b], "col", 1 << b)
    s = double(s, 0, low_bit[0], "col", 1)
    s = s.transpose(tuple(range(row_bits - 1, -1, -1)) + (row_bits + 1, row_bits) + (row_bits + 2, row_bits + 3))
    s = s.reshape(tiles_c, fold, TILE, panel)
    s_r = s.reshape(local_rows, panel)
    own_cols = lax.dynamic_index_in_dim(s, high, 1, keepdims=False)

    def across(x, step):
        mask = 1 << step
        pairs = [
            ((c % n_row ^ d) * n_col + c, (c % n_row ^ d ^ mask) * n_col + c)
            for c in range(n_col)
            for d in range(mask)
        ]
        other = lax.ppermute(x, BOTH, pairs)
        return jnp.where(((p ^ low) & mask) != 0, other, x)

    def along(x, before):
        pairs = [
            (r * n_col + h * n_row + r, r * n_col + (1 - h) * n_row + r)
            for r in range(n_row)
            for h in range(2)
        ]
        other = lax.ppermute(x, BOTH, pairs)
        full = join(x, other, high, 1)
        half = full.shape[0] // 2
        full = full.reshape((2, half) + full.shape[1:])
        give = lax.dynamic_index_in_dim(full, 1 - low_bit[0], 0, keepdims=False)
        mine = lax.dynamic_index_in_dim(full, low_bit[0], 0, keepdims=False)
        pairs = [
            (r * n_col + h * n_row + r, r * n_col + h * n_row + (r ^ 1))
            for r in range(n_row)
            for h in range(2)
        ]
        (give, mine), _ = lax.optimization_barrier(((give, mine), before))
        got = lax.ppermute(give, BOTH, pairs)
        mine = jnp.where(low == p, mine, got)
        first = mine
        held = [0, 1]
        for b in range(1, row_bits):
            mask = 1 << b
            pairs = [
                (r * n_col + h * n_row + (r ^ d), r * n_col + h * n_row + (r ^ d ^ mask))
                for r in range(n_row)
                for h in range(2)
                for d in held
            ]
            got = lax.ppermute(mine, BOTH, pairs)
            mine = jnp.where(((p ^ low) & mask) != 0, got, mine)
            held = held + [d ^ mask for d in held]
        whole = double(mine, 0, low_bit[0], "col", 1)
        return whole.reshape(local_rows, panel), first

    stored = relay(matrix, sent[:streams])
    lead_rows, lead_cols = stored[:top_r], stored[:, :edge_c]
    if panel_tiles % n_row == 0 and panel_tiles % n_col == 0:
        per_r, per_c = panel // n_row, panel // n_col
        piece = lead_cols[:, per_c : 2 * per_c].T.reshape(per_c // TILE, TILE, local_rows)
        piece = double(piece, 1, high, "col", n_row)
        for b in range(row_bits - 1, -1, -1):
            piece = double(piece, 1 + row_bits - b, low_bit[b], "col", 1 << b)
        next_rt = piece.reshape(panel, local_rows)
        piece = lead_rows[per_r : 2 * per_r, :].reshape(per_r // TILE, TILE, local_cols)
        for i, b in enumerate(range(row_bits - 1, -1, -1)):
            piece = double(piece, 1 + i, row_bit[b], "row", 1 << b)
        next_ct = piece.reshape(panel, local_cols)
    else:
        next_rt = lax.psum(mm(lead_cols[:, :top_c], c1), "col").T
        next_ct = lax.psum(mm_t(r1, lead_rows), "row")

    p_c, small, sl_r = product(stored, s_r, under_r, r1)
    small = sum_over(small, "row", 2)
    halves = list(jnp.split(p_c, 2, axis=0))
    for step in range(row_bits):
        for k in range(2):
            halves[k] = halves[k] + swap(halves[k], "row", 1 << ((step + k) % row_bits))
    gram, s_next = small[:panel], small[panel:]
    inv = square_call(factor_kernel, gram)
    halves, inv = lax.optimization_barrier((halves, inv))
    inverse = square_call(shifted_kernel, inv, s_next)
    p_c = jnp.concatenate(halves, axis=0)

    def top_set(x, under, fixed):
        width = under.shape[0]
        return x.at[:width].set(jnp.where(under > 0.5, fixed, x[:width]))

    def less(x, one_hot):
        return x.at[: one_hot.shape[0]].add(-one_hot)

    z_c = mm_nt(p_c, inv, HIGH) - next_ct.T
    z_c = top_set(z_c, under_c, mm_nt(mm(c0[:width_c], gram), inv) - mm_nt(c0[:width_c], s_next))
    s_own = top_set(own_cols.reshape(local_cols, panel), under_c, 0.0)
    y_own = less(mm_nt(s_own, inv, HIGH), c1)
    s_c, y_own, _ = lax.optimization_barrier((own_cols, y_own, p_c))
    wmat = jnp.where(p == low, mm_t(y_own, z_c), 0.0)
    p_r, _ = along(p_c.reshape(tiles_c, TILE, panel), wmat)
    wmat = sum_masks(wmat, "col", [1 << b for b in range(row_bits - 1, 0, -1)] + [n_row])
    wmat = wmat + swap(wmat, "col", 1)
    wmat = sum_masks(wmat, "row", [1 << b for b in range(row_bits)])

    for step in range(row_bits):
        s_c = across(s_c, step)
    s_c = s_c.reshape(local_cols, panel)
    y_c = less(mm_nt(top_set(s_c, under_c, 0.0), inv, HIGH), c1)

    half_core = 0.5 * mm_nt(mm(inverse, wmat), inverse)
    v_c = mm_nt(z_c, inverse, HIGH) - mm(y_c, half_core, HIGH)
    y_r = mm_nt(sl_r, inv, HIGH)
    r_r = mm_t(next_rt, inverse.T, HIGH) + mm(y_r, half_core, HIGH)
    r_r = top_set(r_r, under_r, mm_nt(mm_nt(r0, s_next), inverse))

    left = mm_nt(s_r, c0)
    edge_cols = jnp.where(lane_c[:1] > 0.5, left, lead_cols)
    upper = mm_nt(r0, s_c)
    in_r = under_r[:, :1] > 0.5
    corner = jnp.where(
        in_r,
        jnp.where(lane_c[:1] > 0.5, 0.5 * (left[:width_r] + upper[:, :edge_c]), upper[:, :edge_c]),
        edge_cols[:width_r],
    )
    edge_rows = jnp.concatenate(
        [corner, jnp.where(in_r, upper[:, edge_c:], lead_rows[:width_r, edge_c:])], axis=1
    )
    return update(
        matrix.shape,
        stored,
        y_r,
        p_r,
        r_r,
        under_r,
        mm(r0, gram),
        r1,
        half_core,
        mm_t(inv, inverse.T),
        jnp.concatenate([v_c, y_c], axis=1),
        edge_rows,
        edge_cols,
    )


def solution(mesh):
    in_specs = (
        P(("row", "col"), None),
        P(("row", "col"), None),
        P(("row", "col")),
        P("row", None, "col", None),
    )
    out_specs = P("row", None, "col", None)
    return jax.shard_map(
        step_of, mesh=mesh, in_specs=in_specs, out_specs=out_specs, check_vma=False
    )
```
